32 devices in a mesh: row: 4 (over y, core), col: 8 (over z, x).
Axes of the slice: x: 2, y: 2, z: 4, core: 2. Of those that a mesh axis runs over, the one named last changes fastest.
Arguments:
- demand: bfloat16 [12288, 128], P(('row', 'col')), may hold values from -6 to 6
- tile_data: bfloat16 [4, 8, 128, 128, 128], P('row', 'col'), may hold values from -0.078125 to 0.078125
- tile_row: int32 [4, 8, 128], P('row', 'col'), may hold values from 0 to 12, as said below
- tile_col: int32 [4, 8, 128], P('row', 'col'), may hold values from 0 to 23, as said below
Outputs:
- leontief: bfloat16 [12288, 128], P(('row', 'col'))
The draws below stay inside these ranges and needn't reach their ends.
Inputs may be any that keep to these rules, and one draw needn't show every extreme that they name: `tile_row`: the value 4 * 3 marks an empty slot. In every index pair the live slots come first and number at least 42; in every draw some index pair has all 128 slots live. Two slots may name the same tile position; their tiles then add. `tile_col`: empty slots carry a column too, which is ignored.
All inputs are finite; a program needn't handle non-finite values.
Results may differ from the reference program's by a relative error of at most 0.018.
Values may be sent and summed in bfloat16 or wider, within the bound.
A program may use at most 64 MiB of HBM per device.

```python
import jax
import jax.numpy as jnp
from jax import lax

TILE = 128
SPAN = 3
COLS = 128
SLOTS = 128
SECTORS = 12288
N_ROW = 4
N_COL = 8


def draw_tile_row(key, part):
    key_count = jax.random.fold_in(key, 11)
    key_full = jax.random.fold_in(key, 12)
    key_rows = jax.random.fold_in(key, 13)
    counts = jax.random.randint(key_count, (N_ROW, N_COL), SLOTS // 3, SLOTS + 1)
    chosen = jax.random.randint(key_full, (), 0, N_ROW * N_COL)
    flat_index = jnp.arange(N_ROW * N_COL, dtype=jnp.int32).reshape(N_ROW, N_COL)
    counts = jnp.where(flat_index == chosen, SLOTS, counts)
    rows_drawn = jax.random.randint(key_rows, (N_ROW, N_COL, SLOTS), 0, N_ROW * SPAN)
    slot_index = jnp.arange(SLOTS, dtype=jnp.int32)
    live = slot_index[None, None, :] < counts[:, :, None]
    return jnp.where(live, rows_drawn, N_ROW * SPAN).astype(jnp.int32)


def draw_tile_col(key, part):
    key_cols = jax.random.fold_in(key, 21)
    return jax.random.randint(key_cols, (N_ROW, N_COL, SLOTS), 0, N_COL * SPAN).astype(jnp.int32)


def block_levels(stream_key, dims, pieces, least, largest):
    def one(position, blocks):
        steps = jax.random.uniform(jax.random.fold_in(jax.random.fold_in(stream_key, 6), position), (blocks,), jnp.float32, least / len(pieces), largest / len(pieces))
        return jnp.repeat(jnp.exp(steps), dims[position] // blocks).reshape((-1,) + (1,) * (len(dims) - position - 1))

    gain = one(*pieces[0])
    for cut in pieces[1:]:
        gain = gain * one(*cut)
    return gain


def noise(key, dims, deviation, bound, split=(), kind=jnp.bfloat16):
    drawn = deviation * jax.random.normal(key, dims, jnp.float32)
    if split:
        drawn = drawn * block_levels(key, dims, split, -0.22, 0.18)
    return jnp.clip(drawn, -bound, bound).astype(kind)


def setup_inputs(seed: int = 0) -> dict:
    key_of = jax.random.split(jax.random.key(seed), 5)
    demand = noise(key_of[0], (SECTORS, COLS), 1.0, 6.0, ((0, 32),))
    tile_data = noise(key_of[1], (N_ROW, N_COL, SLOTS, TILE, TILE), (SLOTS * TILE // SPAN) ** -0.5, 0.078125, ((0, 4), (1, 8)))
    tile_row = draw_tile_row(jax.random.fold_in(key_of[4], 71), 0)
    tile_col = draw_tile_col(jax.random.fold_in(key_of[4], 71), 0)
    return {"demand": demand, "tile_data": tile_data, "tile_row": tile_row, "tile_col": tile_col}


def multiply(panel, tile_data, tile_row, tile_col):
    columns = panel.shape[1]
    local_rows = N_ROW * SPAN
    blocks = panel.reshape(N_ROW, N_COL * SPAN, TILE, columns)
    targets = jnp.arange(local_rows, dtype=jnp.int32)

    def per_target(target):
        def accumulate(running, source):
            picked = jnp.take(blocks[source], tile_col[source, target], axis=0)
            products = jnp.einsum("stk,skc->stc", tile_data[source, target].astype(jnp.float32), picked.astype(jnp.float32))
            onehot = (tile_row[source, target][None, :] == targets[:, None]).astype(jnp.float32)
            partial_value = jnp.dot(onehot, products.reshape(SLOTS, -1), precision=lax.Precision.HIGHEST)
            partial_value = lax.optimization_barrier(partial_value.astype(jnp.bfloat16)).astype(jnp.float32)
            return running + partial_value, None

        running, _ = lax.scan(accumulate, jnp.zeros((local_rows, TILE * columns), jnp.float32), jnp.arange(N_ROW, dtype=jnp.int32))
        return running.astype(jnp.bfloat16).reshape(N_ROW, SPAN * TILE, columns)

    stacked = lax.map(per_target, jnp.arange(N_COL, dtype=jnp.int32))
    return stacked.transpose(1, 0, 2, 3).reshape(-1, columns)


def reference(demand, tile_data, tile_row, tile_col):
    first_term = multiply(demand, tile_data, tile_row, tile_col)
    second_term = multiply(first_term, tile_data, tile_row, tile_col)
    summed = demand.astype(jnp.float32) + first_term.astype(jnp.float32) + second_term.astype(jnp.float32)
    return summed.astype(jnp.bfloat16)
```

```python
import functools

import jax
import jax.numpy as jnp
from jax import lax
from jax.experimental import pallas as pl
from jax.experimental.pallas import tpu as pltpu
from jax.sharding import PartitionSpec as P

CHUNKS = 4
BUILD = 8
MESH = pl.DeviceIdType.MESH


def schedule(rows_ref, cols_ref, plan_vector, local_rows, source_tiles):
    slots = rows_ref.shape[1]
    width = plan_vector.shape[1]
    square, wide = (slots, slots), (slots, width)
    key_lane = jnp.broadcast_to(rows_ref[...] * source_tiles + cols_ref[...], square)
    key_sub = jnp.transpose(key_lane)
    lane = lax.broadcasted_iota(jnp.int32, square, 1)
    sub = lax.broadcasted_iota(jnp.int32, square, 0)
    prior = (key_lane == key_sub) & (lane < sub)
    place = jnp.sum(jnp.where((key_lane < key_sub) | prior, 1, 0), axis=1, keepdims=True)
    repeats = jnp.sum(jnp.where(prior, 1, 0), axis=1, keepdims=True)
    hit = jnp.broadcast_to(place, square) == lane

    def total(value):
        return jnp.sum(jnp.where(hit, value, 0), axis=0, keepdims=True)

    spot = lax.broadcasted_iota(jnp.int32, wide, 1)
    here = jnp.broadcast_to(key_sub[:, 0:1], wide) == spot
    last = jnp.max(jnp.where(here, jnp.broadcast_to(place, wide), -1), axis=0, keepdims=True)
    plan_vector[0:1, :] = jnp.where(last < 0, slots, last)
    plan_vector[1:2, 0:slots] = total(sub)
    plan_vector[2:3, 0:slots] = total(jnp.broadcast_to(jnp.where(repeats == 0, 0, 1), square))


def order_of(chunks):
    ops = [("Z", 0, 0), ("S", 0, 0)]
    for c in range(1, chunks):
        ops += [("Z", 0, c), ("X", 0, c - 1), ("S", 0, c)]
        if c >= 3:
            ops += [("E", 0, c - 3)]
    ops += [("X", 0, chunks - 1)]
    ops += [("E", 0, c) for c in range(max(chunks - 3, 0), chunks - 1)]
    ops += [("Z", 1, 0), ("S", 1, 0), ("E", 0, chunks - 1)]
    for c in range(1, chunks):
        ops += [("Z", 1, c), ("X", 1, c - 1), ("S", 1, c)]
        if c >= 3:
            ops += [("E", 1, c - 3)]
    ops += [("X", 1, chunks - 1)]
    ops += [("E", 1, c) for c in range(max(chunks - 3, 0), chunks)]
    return ops


def kernel(n_row, n_col, n_x, rows_ref, cols_ref, demand, tile_hbm, out, tiles, weights, panel_a, panel_b, sums,
           packed, landed, out_turned, plan_vector, plan, tile_sem, plan_sem, sx, rx, sz, rz, sr, rr):
    n_z = n_col // n_x
    span, edge, columns = demand.shape
    slots = tiles.shape[0]
    source_tiles = n_col * span
    local_rows = n_row * span
    panels = (panel_a, panel_b)
    chunks, part = panel_a.shape[0], panel_a.shape[2]
    row = lax.axis_index("row")
    col = lax.axis_index("col")
    z = col // n_x
    x = col % n_x
    other = n_x - 1 - x
    paired = n_z & (n_z - 1) == 0
    cores = 2 if n_row % 2 == 0 else 1
    n_y = n_row // cores

    tile_copy = pltpu.make_async_copy(tile_hbm.at[0, 0], tiles, tile_sem)
    tile_copy.start()

    def flipped(value, k):
        bit, result = 1, value
        while bit <= k:
            if k & bit:
                result = result + bit - 2 * bit * ((value // bit) % 2)
            bit *= 2
        return result

    def sent_to(k):
        return flipped(z, k) if paired else (z + k) % n_z

    def got_from(k):
        return flipped(z, k) if paired else (z + n_z - k) % n_z

    def target(e):
        return ((row // cores + 1 + e // cores) % n_y) * cores + (row % cores + 1 + e % cores) % cores

    barrier = pltpu.get_barrier_semaphore()

    def greet(r, c):
        pl.semaphore_signal(barrier, inc=1, device_id=(r, c), device_id_type=MESH)

    for k in range(1, n_z):
        greet(row, sent_to(k) * n_x + x)
    for e in range(n_row - 1):
        greet(target(e), col)
    if n_x > 1:
        greet(row, z * n_x + other)

    for k in range(span):
        turned = jnp.transpose(demand[k])
        for c in range(chunks):
            panel_a[c, col * span + k] = turned[c * part:(c + 1) * part]
    pl.semaphore_wait(barrier, n_z - 1 + n_row - 1 + (1 if n_x > 1 else 0))

    def block(p, c, zz, xx):
        return panels[p].at[c, pl.ds((zz * n_x + xx) * span, span)]

    def remote(src, dst, send, recv, device):
        return pltpu.make_async_remote_copy(
            src_ref=src, dst_ref=dst, send_sem=send, recv_sem=recv, device_id=device, device_id_type=MESH
        )

    def across(p, c, k):
        here = block(p, c, got_from(k) if k else z, x)
        return remote(here, here, sx.at[p, c, k], rx.at[p, c, k], (row, z * n_x + other))

    def across_in(p, c, k):
        here = block(p, c, got_from(k) if k else z, other)
        remote(here, here, sx.at[p, c, k], rx.at[p, c, k], (row, z * n_x + other)).wait_recv()

    def along(p, c, k):
        here = block(p, c, z, x)
        return remote(here, here, sz.at[p, c, k - 1], rz.at[p, c, k - 1], (row, sent_to(k) * n_x + x))

    def along_in(p, c, k):
        here = block(p, c, got_from(k), x)
        remote(here, here, sz.at[p, c, k - 1], rz.at[p, c, k - 1], (row, sent_to(k) * n_x + x)).wait_recv()

    def reduce_copy(p, c, e):
        return remote(packed.at[p, c, pl.ds(e * span, span)], landed.at[p, c, e], sr.at[p, c, e], rr.at[p, c, e],
                      (target(e), col))

    def launch(p, c):
        if n_x > 1:
            across(p, c, 0).start()
        for k in reversed(range(1, n_z)):
            along(p, c, k).start()

    def relay(p, c):
        for k in range(1, n_z):
            along_in(p, c, k)
            if n_x > 1:
                across(p, c, k).start()

    def product(p, c, sources, first, final):
        held = [block_tile for source in sources for block_tile in [source * span + k for k in range(span)]]
        deep = [held[i:i + 2] for i in range(0, len(held), 2)]
        left = [jnp.concatenate([panels[p][c, t] for t in group], axis=1) for group in deep]

        def unit(u):
            places = [u * cores * span + q for q in range(cores * span)]
            for at in range(0, len(places), 2):
                pair = places[at:at + 2]
                home = [target(q // span) * span + q % span for q in pair]
                total = None
                for group, value in zip(deep, left):
                    right = jnp.concatenate(
                        [jnp.concatenate([weights[plan[0, h * source_tiles + t]] for t in group], axis=0) for h in home],
                        axis=1,
                    )
                    term = jnp.dot(value, right, preferred_element_type=jnp.float32)
                    total = term if total is None else total + term
                for i, q in enumerate(pair):
                    value = total[:, i * edge:(i + 1) * edge]
                    if not first:
                        value = value + sums[c, q]
                    static = isinstance(q, int)
                    if not final or not static or q >= (n_row - 1) * span:
                        sums[c, q] = value
                    if final and (not static or q < (n_row - 1) * span):
                        packed[p, c, q] = value.astype(packed.dtype)
            if final:
                for i in range(cores):
                    e = u * cores + i
                    if isinstance(e, int):
                        if e < n_row - 1:
                            reduce_copy(p, c, e).start()
                    else:
                        pl.when(e < n_row - 1)(lambda: reduce_copy(p, c, e).start())

        if n_y <= 2:
            for u in range(n_y):
                unit(u)
        else:
            lax.fori_loop(0, n_y, lambda u, _: (unit(u), 0)[1], 0)

    def near(p, c):
        product(p, c, [(got_from(k) if k else z) * n_x + x for k in range(n_z)], True, n_x == 1)

    def far(p, c):
        if n_x > 1:
            half = n_z // 2 if n_z > 1 else n_z
            for lo, hi in ((0, half), (half, n_z)):
                if lo < hi:
                    for k in range(lo, hi):
                        across_in(p, c, k)
                    product(p, c, [(got_from(k) if k else z) * n_x + other for k in range(lo, hi)], False, hi == n_z)

    def collect(p, c):
        for e in range(n_row - 1):
            reduce_copy(p, c, e).wait_recv()
        for k in range(span):
            value = sums[c, (n_row - 1) * span + k]
            for e in range(n_row - 1):
                value = value + landed[p, c, e, k].astype(jnp.float32)
            value = value.astype(panel_b.dtype)
            mine = col * span + k
            if p == 0:
                panel_b[c, mine] = value
            else:
                out_turned[k, c * part:(c + 1) * part] = (
                    panel_a[c, mine].astype(jnp.float32) + panel_b[c, mine].astype(jnp.float32)
                    + value.astype(jnp.float32)
                ).astype(out.dtype)
        if p == 0:
            launch(1, c)

    for c in range(chunks):
        launch(0, c)

    schedule(rows_ref, cols_ref, plan_vector, local_rows, source_tiles)
    plan_copy = pltpu.make_async_copy(plan_vector, plan, plan_sem)
    plan_copy.start()
    weights[slots] = jnp.zeros((edge, edge), weights.dtype)
    plan_copy.wait()
    tile_copy.wait()

    def merge(step, total):
        for u in range(BUILD):
            at = step * BUILD + u
            keep = plan[2, at].astype(jnp.float32)
            total = total * keep + tiles[plan[1, at]].astype(jnp.float32)
            weights[at] = jnp.transpose(total.astype(weights.dtype))
        return total

    lax.fori_loop(0, slots // BUILD, merge, jnp.zeros((edge, edge), jnp.float32))

    act = {"Z": relay, "S": near, "X": far, "E": collect}
    for op, p, c in order_of(chunks):
        act[op](p, c)

    for k in range(span):
        out[k] = jnp.transpose(out_turned[k])
    for p in range(2):
        for c in range(chunks):
            for k in range(n_z):
                if n_x > 1:
                    across(p, c, k).wait_send()
                if k:
                    along(p, c, k).wait_send()
            for e in range(n_row - 1):
                reduce_copy(p, c, e).wait_send()


def body(n_row, n_col, demand, tile_data, tile_row, tile_col):
    slots, edge = tile_data.shape[2], tile_data.shape[-1]
    columns = demand.shape[1]
    span = demand.shape[0] // edge
    local_rows = n_row * span
    n_x = 2 if n_col % 2 == 0 else 1
    n_z = n_col // n_x
    part = columns // CHUNKS
    width = -(-max(local_rows * n_col * span, slots) // 128) * 128
    dma = pltpu.SemaphoreType.DMA
    kind = demand.dtype
    vmem = pl.BlockSpec(memory_space=pltpu.VMEM)
    result = pl.pallas_call(
        functools.partial(kernel, n_row, n_col, n_x),
        out_shape=jax.ShapeDtypeStruct((span, edge, columns), kind),
        in_specs=[vmem, vmem, vmem, pl.BlockSpec(memory_space=pl.ANY)],
        out_specs=vmem,
        scratch_shapes=[
            pltpu.VMEM((slots, edge, edge), tile_data.dtype),
            pltpu.VMEM((slots + 1, edge, edge), tile_data.dtype),
            pltpu.VMEM((CHUNKS, n_col * span, part, edge), kind),
            pltpu.VMEM((CHUNKS, n_col * span, part, edge), kind),
            pltpu.VMEM((CHUNKS, local_rows, part, edge), jnp.float32),
            pltpu.VMEM((2, CHUNKS, local_rows, part, edge), kind),
            pltpu.VMEM((2, CHUNKS, n_row - 1, span, part, edge), kind),
            pltpu.VMEM((span, columns, edge), kind),
            pltpu.VMEM((8, width), jnp.int32),
            pltpu.SMEM((8, width), jnp.int32),
            dma,
            dma,
            dma((2, CHUNKS, n_z)),
            dma((2, CHUNKS, n_z)),
            dma((2, CHUNKS, n_z)),
            dma((2, CHUNKS, n_z)),
            dma((2, CHUNKS, n_row - 1)),
            dma((2, CHUNKS, n_row - 1)),
        ],
        compiler_params=pltpu.CompilerParams(
            collective_id=0, has_side_effects=True, vmem_limit_bytes=56 * 1024 * 1024
        ),
    )(tile_row[0], tile_col[0], demand.reshape(span, edge, columns), tile_data)
    return result.reshape(demand.shape)


def solution(mesh):
    placed = (
        P(("row", "col"), None),
        P("row", "col", None, None, None),
        P("row", "col", None),
        P("row", "col", None),
    )
    return jax.shard_map(
        functools.partial(body, mesh.shape["row"], mesh.shape["col"]),
        mesh=mesh, in_specs=placed, out_specs=P(("row", "col"), None), check_vma=False,
    )
```

```python
import functools

import jax
import jax.numpy as jnp
from jax import lax
from jax.experimental import pallas as pl
from jax.experimental.pallas import tpu as pltpu
from jax.sharding import PartitionSpec as P

CHUNKS = 4
BUILD = 8
EARLY = 6
ORDER = (
    "Z002", "Z000", "Z001", "S001", "Z010", "Z011", "Z012", "S011", "Z022", "X000", "X001",
    "Z021", "Z020", "S021", "X010", "Z032", "Z031", "X011", "Z030", "S031", "E000", "X020",
    "X021", "E010", "X030", "X031", "E020", "Z100", "Z102", "Z101", "S101", "Z110", "Z112",
    "E030", "Z111", "S111", "Z121", "X100", "X101", "Z120", "Z122", "X110", "Z130", "X111",
    "Z131", "Z132", "S121", "S131", "X120", "X121", "X130", "X131", "E110", "E100", "E120",
    "E130",
)
MESH = pl.DeviceIdType.MESH


def schedule(rows_ref, cols_ref, plan_vector, local_rows, source_tiles):
    slots = rows_ref.shape[1]
    width = plan_vector.shape[1]
    square, wide = (slots, slots), (slots, width)
    key_lane = jnp.broadcast_to(rows_ref[...] * source_tiles + cols_ref[...], square)
    key_sub = jnp.transpose(key_lane)
    lane = lax.broadcasted_iota(jnp.int32, square, 1)
    sub = lax.broadcasted_iota(jnp.int32, square, 0)
    prior = (key_lane == key_sub) & (lane < sub)
    place = jnp.sum(jnp.where((key_lane < key_sub) | prior, 1, 0), axis=1, keepdims=True)
    repeats = jnp.sum(jnp.where(prior, 1, 0), axis=1, keepdims=True)
    hit = jnp.broadcast_to(place, square) == lane

    def total(value):
        return jnp.sum(jnp.where(hit, value, 0), axis=0, keepdims=True)

    spot = lax.broadcasted_iota(jnp.int32, wide, 1)
    here = jnp.broadcast_to(key_sub[:, 0:1], wide) == spot
    last = jnp.max(jnp.where(here, jnp.broadcast_to(place, wide), -1), axis=0, keepdims=True)
    plan_vector[0:1, :] = jnp.where(last < 0, slots, last)
    plan_vector[1:2, 0:slots] = total(sub)
    plan_vector[2:3, 0:slots] = total(jnp.broadcast_to(jnp.where(repeats == 0, 0, 1), square))


def order_of():
    return [(word[0], int(word[1]), int(word[2]), int(word[3])) for word in ORDER]


def kernel(n_row, n_col, n_x, rows_hbm, cols_hbm, demand_hbm, tile_hbm, out, rows_ref, cols_ref, demand, tiles, weights, panel_a, panel_b, sums,
           packed, landed, out_turned, plan_vector, plan, copy_sem, plan_sem, sx, rx, sz, rz, sr, rr):
    n_z = n_col // n_x
    span, edge, columns = demand.shape
    slots = tiles.shape[0]
    source_tiles = n_col * span
    local_rows = n_row * span
    panels = (panel_a, panel_b)
    chunks, part = panel_a.shape[0], panel_a.shape[2]
    row = lax.axis_index("row")
    col = lax.axis_index("col")
    z = col // n_x
    x = col % n_x
    other = n_x - 1 - x
    paired = n_z & (n_z - 1) == 0
    cores = 2 if n_row % 2 == 0 else 1
    n_y = n_row // cores

    copies = [
        pltpu.make_async_copy(source, there, copy_sem.at[i])
        for i, (source, there) in enumerate(
            ((demand_hbm, demand), (rows_hbm, rows_ref), (cols_hbm, cols_ref), (tile_hbm.at[0, 0], tiles))
        )
    ]
    demand_copy, rows_copy, cols_copy, tile_copy = copies
    for copy in copies:
        copy.start()

    def flipped(value, k):
        bit, result = 1, value
        while bit <= k:
            if k & bit:
                result = result + bit - 2 * bit * ((value // bit) % 2)
            bit *= 2
        return result

    def sent_to(k):
        return flipped(z, k) if paired else (z + k) % n_z

    def got_from(k):
        return flipped(z, k) if paired else (z + n_z - k) % n_z

    def target(e):
        return ((row // cores + 1 + e // cores) % n_y) * cores + (row % cores + 1 + e % cores) % cores

    barrier = pltpu.get_barrier_semaphore()

    def greet(r, c):
        pl.semaphore_signal(barrier, inc=1, device_id=(r, c), device_id_type=MESH)

    for k in range(1, n_z):
        greet(row, sent_to(k) * n_x + x)
    for e in range(n_row - 1):
        greet(target(e), col)
    if n_x > 1:
        greet(row, z * n_x + other)

    rows_copy.wait()
    cols_copy.wait()
    schedule(rows_ref, cols_ref, plan_vector, local_rows, source_tiles)
    plan_copy = pltpu.make_async_copy(plan_vector, plan, plan_sem)
    plan_copy.start()
    weights[slots] = jnp.zeros((edge, edge), weights.dtype)
    demand_copy.wait()
    for k in range(span):
        turned = jnp.transpose(demand[k])
        for c in range(chunks):
            panel_a[c, col * span + k] = turned[c * part:(c + 1) * part]
    plan_copy.wait()
    tile_copy.wait()

    def merge(step, total):
        for u in range(BUILD):
            at = step * BUILD + u
            keep = plan[2, at].astype(jnp.float32)
            total = total * keep + tiles[plan[1, at]].astype(jnp.float32)
            weights[at] = jnp.transpose(total.astype(weights.dtype))
        return total

    steps = slots // BUILD
    early = steps * EARLY // 8
    running = lax.fori_loop(0, early, merge, jnp.zeros((edge, edge), jnp.float32))
    pl.semaphore_wait(barrier, n_z - 1 + n_row - 1 + (1 if n_x > 1 else 0))

    def block(p, c, zz, xx):
        return panels[p].at[c, pl.ds((zz * n_x + xx) * span, span)]

    def remote(src, dst, send, recv, device):
        return pltpu.make_async_remote_copy(
            src_ref=src, dst_ref=dst, send_sem=send, recv_sem=recv, device_id=device, device_id_type=MESH
        )

    def across(p, c, k):
        here = block(p, c, got_from(k) if k else z, x)
        return remote(here, here, sx.at[p, c, k], rx.at[p, c, k], (row, z * n_x + other))

    def across_in(p, c, k):
        here = block(p, c, got_from(k) if k else z, other)
        remote(here, here, sx.at[p, c, k], rx.at[p, c, k], (row, z * n_x + other)).wait_recv()

    def along(p, c, k):
        here = block(p, c, z, x)
        return remote(here, here, sz.at[p, c, k - 1], rz.at[p, c, k - 1], (row, sent_to(k) * n_x + x))

    def along_in(p, c, k):
        here = block(p, c, got_from(k), x)
        remote(here, here, sz.at[p, c, k - 1], rz.at[p, c, k - 1], (row, sent_to(k) * n_x + x)).wait_recv()

    def reduce_copy(p, c, e):
        return remote(packed.at[p, c, pl.ds(e * span, span)], landed.at[p, c, e], sr.at[p, c, e], rr.at[p, c, e],
                      (target(e), col))

    def launch(p, c):
        if n_x > 1:
            across(p, c, 0).start()
        for k in reversed(range(1, n_z)):
            along(p, c, k).start()

    def relay(p, c, at):
        for k in range(1, n_z)[(n_z - 1) * at // 3:(n_z - 1) * (at + 1) // 3]:
            along_in(p, c, k)
            if n_x > 1:
                across(p, c, k).start()

    def product(p, group, sources, first, final):
        held = [block_tile for source in sources for block_tile in [source * span + k for k in range(span)]]
        deep = [held[i:i + 2] for i in range(0, len(held), 2)]
        left = [
            jnp.concatenate([jnp.concatenate([panels[p][c, t] for t in near], axis=1) for c in group], axis=0)
            for near in deep
        ]

        def unit(u):
            places = [u * cores * span + q for q in range(cores * span)]
            for at in range(0, len(places), 2):
                pair = places[at:at + 2]
                home = [target(q // span) * span + q % span for q in pair]
                total = None
                for near, value in zip(deep, left):
                    right = jnp.concatenate(
                        [jnp.concatenate([weights[plan[0, h * source_tiles + t]] for t in near], axis=0) for h in home],
                        axis=1,
                    )
                    term = jnp.dot(value, right, preferred_element_type=jnp.float32)
                    total = term if total is None else total + term
                for i, q in enumerate(pair):
                    for j, c in enumerate(group):
                        value = total[j * part:(j + 1) * part, i * edge:(i + 1) * edge]
                        if not first:
                            value = value + sums[c, q]
                        static = isinstance(q, int)
                        if not final or not static or q >= (n_row - 1) * span:
                            sums[c, q] = value
                        if final and (not static or q < (n_row - 1) * span):
                            packed[p, c, q] = value.astype(packed.dtype)
            if final:
                for i, c in [(i, c) for i in range(cores) for c in group]:
                    e = u * cores + i
                    if isinstance(e, int):
                        if e < n_row - 1:
                            reduce_copy(p, c, e).start()
                    else:
                        pl.when(e < n_row - 1)(functools.partial(lambda c, e: reduce_copy(p, c, e).start(), c, e))

        if n_y <= 2:
            for u in range(n_y):
                unit(u)
        else:
            lax.fori_loop(0, n_y, lambda u, _: (unit(u), 0)[1], 0)

    def near(p, c, at):
        product(p, range(c, c + at), [(got_from(k) if k else z) * n_x + x for k in range(n_z)], True, n_x == 1)

    def far(p, c, at):
        lo, hi = n_z * at // 2, n_z * (at + 1) // 2
        if n_x > 1 and lo < hi:
            for k in range(lo, hi):
                across_in(p, c, k)
            product(p, [c], [(got_from(k) if k else z) * n_x + other for k in range(lo, hi)], False, hi == n_z)

    def collect(p, c, at):
        for e in range(n_row - 1):
            reduce_copy(p, c, e).wait_recv()
        for k in range(span):
            value = sums[c, (n_row - 1) * span + k]
            for e in range(n_row - 1):
                value = value + landed[p, c, e, k].astype(jnp.float32)
            value = value.astype(panel_b.dtype)
            mine = col * span + k
            if p == 0:
                panel_b[c, mine] = value
            else:
                out_turned[k, c * part:(c + 1) * part] = (
                    panel_a[c, mine].astype(jnp.float32) + panel_b[c, mine].astype(jnp.float32)
                    + value.astype(jnp.float32)
                ).astype(out.dtype)
        if p == 0:
            launch(1, c)

    for c in range(chunks):
        launch(0, c)

    if early < steps:
        lax.fori_loop(early, steps, merge, running)

    act = {"Z": relay, "S": near, "X": far, "E": collect}
    for op, p, c, at in order_of():
        act[op](p, c, at)

    for k in range(span):
        out[k] = jnp.transpose(out_turned[k])
    for p in range(2):
        for c in range(chunks):
            for k in range(n_z):
                if n_x > 1:
                    across(p, c, k).wait_send()
                if k:
                    along(p, c, k).wait_send()
            for e in range(n_row - 1):
                reduce_copy(p, c, e).wait_send()


def body(n_row, n_col, demand, tile_data, tile_row, tile_col):
    slots, edge = tile_data.shape[2], tile_data.shape[-1]
    columns = demand.shape[1]
    span = demand.shape[0] // edge
    local_rows = n_row * span
    n_x = 2 if n_col % 2 == 0 else 1
    n_z = n_col // n_x
    part = columns // CHUNKS
    width = -(-max(local_rows * n_col * span, slots) // 128) * 128
    dma = pltpu.SemaphoreType.DMA
    kind = demand.dtype
    vmem = pl.BlockSpec(memory_space=pltpu.VMEM)
    result = pl.pallas_call(
        functools.partial(kernel, n_row, n_col, n_x),
        out_shape=jax.ShapeDtypeStruct((span, edge, columns), kind),
        in_specs=[pl.BlockSpec(memory_space=pl.ANY)] * 4,
        out_specs=vmem,
        scratch_shapes=[
            pltpu.VMEM((1, slots), jnp.int32),
            pltpu.VMEM((1, slots), jnp.int32),
            pltpu.VMEM((span, edge, columns), kind),
            pltpu.VMEM((slots, edge, edge), tile_data.dtype),
            pltpu.VMEM((slots + 1, edge, edge), tile_data.dtype),
            pltpu.VMEM((CHUNKS, n_col * span, part, edge), kind),
            pltpu.VMEM((CHUNKS, n_col * span, part, edge), kind),
            pltpu.VMEM((CHUNKS, local_rows, part, edge), jnp.float32),
            pltpu.VMEM((2, CHUNKS, local_rows, part, edge), kind),
            pltpu.VMEM((2, CHUNKS, n_row - 1, span, part, edge), kind),
            pltpu.VMEM((span, columns, edge), kind),
            pltpu.VMEM((8, width), jnp.int32),
            pltpu.SMEM((8, width), jnp.int32),
            dma((4,)),
            dma,
            dma((2, CHUNKS, n_z)),
            dma((2, CHUNKS, n_z)),
            dma((2, CHUNKS, n_z)),
            dma((2, CHUNKS, n_z)),
            dma((2, CHUNKS, n_row - 1)),
            dma((2, CHUNKS, n_row - 1)),
        ],
        compiler_params=pltpu.CompilerParams(
            collective_id=0, has_side_effects=True, vmem_limit_bytes=28 * 1024 * 1024
        ),
    )(*(
        pltpu.with_memory_space_constraint(operand, pltpu.HBM)
        for operand in (tile_row[0], tile_col[0], demand.reshape(span, edge, columns), tile_data)
    ))
    return result.reshape(demand.shape)


def solution(mesh):
    placed = (
        P(("row", "col"), None),
        P("row", "col", None, None, None),
        P("row", "col", None),
        P("row", "col", None),
    )
    return jax.shard_map(
        functools.partial(body, mesh.shape["row"], mesh.shape["col"]),
        mesh=mesh, in_specs=placed, out_specs=P(("row", "col"), None), check_vma=False,
    )
```

```python
import functools

import jax
import jax.numpy as jnp
from jax import lax
from jax.experimental import pallas as pl
from jax.experimental.pallas import tpu as pltpu
from jax.sharding import PartitionSpec as P

CHUNKS = 4
BUILD = 8
ORDER = (
    "Z002", "Z000", "Z001", "S001", "Z010", "Z011", "Z012", "S011", "Z022", "X000", "X001",
    "Z021", "Z020", "S021", "X010", "Z032", "Z031", "X011", "Z030", "S031", "E000", "X020",
    "X021", "E010", "X030", "X031", "E020", "Z100", "Z102", "Z101", "S101", "Z110", "Z112",
    "E030", "Z111", "S111", "Z121", "X100", "X101", "Z120", "Z122", "X110", "Z130", "X111",
    "Z131", "Z132", "S121", "S131", "X120", "X121", "X130", "X131", "E110", "E100", "E120",
    "E130",
)
MESH = pl.DeviceIdType.MESH


def schedule(rows_ref, cols_ref, plan_vector, local_rows, source_tiles):
    slots = rows_ref.shape[1]
    width = plan_vector.shape[1]
    square, wide = (slots, slots), (slots, width)
    key_lane = jnp.broadcast_to(rows_ref[...] * source_tiles + cols_ref[...], square)
    key_sub = jnp.transpose(key_lane)
    lane = lax.broadcasted_iota(jnp.int32, square, 1)
    sub = lax.broadcasted_iota(jnp.int32, square, 0)
    prior = (key_lane == key_sub) & (lane < sub)
    place = jnp.sum(jnp.where((key_lane < key_sub) | prior, 1, 0), axis=1, keepdims=True)
    repeats = jnp.sum(jnp.where(prior, 1, 0), axis=1, keepdims=True)
    hit = jnp.broadcast_to(place, square) == lane

    def total(value):
        return jnp.sum(jnp.where(hit, value, 0), axis=0, keepdims=True)

    spot = lax.broadcasted_iota(jnp.int32, wide, 1)
    here = jnp.broadcast_to(key_sub[:, 0:1], wide) == spot
    last = jnp.max(jnp.where(here, jnp.broadcast_to(place, wide), -1), axis=0, keepdims=True)
    plan_vector[0:1, :] = jnp.where(last < 0, slots, last)
    plan_vector[1:2, 0:slots] = total(sub)
    plan_vector[2:3, 0:slots] = total(jnp.broadcast_to(jnp.where(repeats == 0, 0, 1), square))


def order_of():
    return [(word[0], int(word[1]), int(word[2]), int(word[3])) for word in ORDER]


def kernel(n_row, n_col, n_x, rows_hbm, cols_hbm, demand_hbm, tile_hbm, out, rows_ref, cols_ref, demand, tiles, weights, panel_a, panel_b, sums,
           packed, landed, out_turned, plan_vector, plan, met, copy_sem, plan_sem, sx, rx, sz, rz, sr, rr):
    n_z = n_col // n_x
    span, edge, columns = demand.shape
    slots = tiles.shape[0]
    source_tiles = n_col * span
    local_rows = n_row * span
    panels = (panel_a, panel_b)
    chunks, part = panel_a.shape[0], panel_a.shape[2]
    row = lax.axis_index("row")
    col = lax.axis_index("col")
    z = col // n_x
    x = col % n_x
    other = n_x - 1 - x
    paired = n_z & (n_z - 1) == 0
    cores = 2 if n_row % 2 == 0 else 1
    n_y = n_row // cores

    copies = [
        pltpu.make_async_copy(source, there, copy_sem.at[i])
        for i, (source, there) in enumerate(
            ((demand_hbm, demand), (rows_hbm, rows_ref), (cols_hbm, cols_ref), (tile_hbm.at[0, 0], tiles))
        )
    ]
    demand_copy, rows_copy, cols_copy, tile_copy = copies
    for copy in copies:
        copy.start()

    def flipped(value, k):
        bit, result = 1, value
        while bit <= k:
            if k & bit:
                result = result + bit - 2 * bit * ((value // bit) % 2)
            bit *= 2
        return result

    def sent_to(k):
        return flipped(z, k) if paired else (z + k) % n_z

    def got_from(k):
        return flipped(z, k) if paired else (z + n_z - k) % n_z

    def target(e):
        return ((row // cores + 1 + e // cores) % n_y) * cores + (row % cores + 1 + e % cores) % cores

    barrier = pltpu.get_barrier_semaphore()

    def greet(r, c):
        pl.semaphore_signal(barrier, inc=1, device_id=(r, c), device_id_type=MESH)

    above, below = z + 1 < n_z, z > 0
    pl.when(above)(lambda: greet(row, col + n_x))
    pl.when(below)(lambda: greet(row, col - n_x))
    for e in range(n_row - 1):
        greet(target(e), col)
    if n_x > 1:
        greet(row, z * n_x + other)

    rows_copy.wait()
    cols_copy.wait()
    schedule(rows_ref, cols_ref, plan_vector, local_rows, source_tiles)
    plan_copy = pltpu.make_async_copy(plan_vector, plan, plan_sem)
    plan_copy.start()
    weights[slots] = jnp.zeros((edge, edge), weights.dtype)
    demand_copy.wait()
    for k in range(span):
        turned = jnp.transpose(demand[k])
        for c in range(chunks):
            panel_a[c, col * span + k] = turned[c * part:(c + 1) * part]
    greeted = n_row - 1 + (1 if n_x > 1 else 0) + above.astype(jnp.int32) + below.astype(jnp.int32)
    pl.semaphore_wait(barrier, greeted)

    def block(p, c, zz, xx):
        return panels[p].at[c, pl.ds((zz * n_x + xx) * span, span)]

    def remote(src, dst, send, recv, device):
        return pltpu.make_async_remote_copy(
            src_ref=src, dst_ref=dst, send_sem=send, recv_sem=recv, device_id=device, device_id_type=MESH
        )

    def across(p, c, k):
        here = block(p, c, got_from(k) if k else z, x)
        return remote(here, here, sx.at[p, c, k], rx.at[p, c, k], (row, z * n_x + other))

    def across_in(p, c, k):
        here = block(p, c, got_from(k) if k else z, other)
        remote(here, here, sx.at[p, c, k], rx.at[p, c, k], (row, z * n_x + other)).wait_recv()

    def along(p, c, zz):
        here = block(p, c, z, x)
        return remote(here, here, sz.at[p, c, zz], rz.at[p, c, z], (row, zz * n_x + x))

    def along_in(p, c, zz):
        here = block(p, c, zz, x)
        remote(here, here, sz.at[p, c, zz], rz.at[p, c, zz], (row, zz * n_x + x)).wait_recv()

    def reduce_copy(p, c, e):
        return remote(packed.at[p, c, pl.ds(e * span, span)], landed.at[p, c, e], sr.at[p, c, e], rr.at[p, c, e],
                      (target(e), col))

    def launch(p, c):
        if n_x > 1:
            across(p, c, 0).start()
        for k in reversed(range(1, n_z)):
            along(p, c, sent_to(k)).start()

    def spread(c, away):
        pl.when(z + away < n_z)(lambda: along(0, c, z + away).start())
        pl.when(z >= away)(lambda: along(0, c, z - away).start())

    def vouch(away):
        @pl.when(above & (z >= away - 1))
        def _():
            pl.semaphore_signal(met.at[0, away], inc=1, device_id=(row, col + n_x), device_id_type=MESH)

        @pl.when(below & (z + away - 1 < n_z))
        def _():
            pl.semaphore_signal(met.at[1, away], inc=1, device_id=(row, col - n_x), device_id_type=MESH)

    def vouched(away):
        pl.when(z >= away)(lambda: pl.semaphore_wait(met.at[0, away], 1))
        pl.when(z + away < n_z)(lambda: pl.semaphore_wait(met.at[1, away], 1))

    def relay(p, c, at):
        for k in range(1, n_z)[(n_z - 1) * at // 3:(n_z - 1) * (at + 1) // 3]:
            along_in(p, c, got_from(k))
            if n_x > 1:
                across(p, c, k).start()

    def product(p, group, sources, first, final):
        held = [block_tile for source in sources for block_tile in [source * span + k for k in range(span)]]
        deep = [held[i:i + 2] for i in range(0, len(held), 2)]
        left = [
            jnp.concatenate([jnp.concatenate([panels[p][c, t] for t in near], axis=1) for c in group], axis=0)
            for near in deep
        ]

        def unit(u):
            places = [u * cores * span + q for q in range(cores * span)]
            for at in range(0, len(places), 2):
                pair = places[at:at + 2]
                home = [target(q // span) * span + q % span for q in pair]
                total = None
                for near, value in zip(deep, left):
                    right = jnp.concatenate(
                        [jnp.concatenate([weights[plan[0, h * source_tiles + t]] for t in near], axis=0) for h in home],
                        axis=1,
                    )
                    term = jnp.dot(value, right, preferred_element_type=jnp.float32)
                    total = term if total is None else total + term
                for i, q in enumerate(pair):
                    for j, c in enumerate(group):
                        value = total[j * part:(j + 1) * part, i * edge:(i + 1) * edge]
                        if not first:
                            value = value + sums[c, q]
                        static = isinstance(q, int)
                        if not final or not static or q >= (n_row - 1) * span:
                            sums[c, q] = value
                        if final and (not static or q < (n_row - 1) * span):
                            packed[p, c, q] = value.astype(packed.dtype)
            if final:
                for i, c in [(i, c) for i in range(cores) for c in group]:
                    e = u * cores + i
                    if isinstance(e, int):
                        if e < n_row - 1:
                            reduce_copy(p, c, e).start()
                    else:
                        pl.when(e < n_row - 1)(functools.partial(lambda c, e: reduce_copy(p, c, e).start(), c, e))

        if n_y <= 2:
            for u in range(n_y):
                unit(u)
        else:
            lax.fori_loop(0, n_y, lambda u, _: (unit(u), 0)[1], 0)

    def near(p, c, at):
        product(p, range(c, c + at), [(got_from(k) if k else z) * n_x + x for k in range(n_z)], True, n_x == 1)

    def far(p, c, at):
        lo, hi = n_z * at // 2, n_z * (at + 1) // 2
        if n_x > 1 and lo < hi:
            for k in range(lo, hi):
                across_in(p, c, k)
            product(p, [c], [(got_from(k) if k else z) * n_x + other for k in range(lo, hi)], False, hi == n_z)

    def collect(p, c, at):
        for e in range(n_row - 1):
            reduce_copy(p, c, e).wait_recv()
        for k in range(span):
            value = sums[c, (n_row - 1) * span + k]
            for e in range(n_row - 1):
                value = value + landed[p, c, e, k].astype(jnp.float32)
            value = value.astype(panel_b.dtype)
            mine = col * span + k
            if p == 0:
                panel_b[c, mine] = value
            else:
                out_turned[k, c * part:(c + 1) * part] = (
                    panel_a[c, mine].astype(jnp.float32) + panel_b[c, mine].astype(jnp.float32)
                    + value.astype(jnp.float32)
                ).astype(out.dtype)
        if p == 0:
            launch(1, c)

    for c in range(chunks):
        if n_x > 1:
            across(0, c, 0).start()
        if n_z > 1 and c == 0:
            spread(c, 1)
    if n_z > 2:
        vouch(2)
    plan_copy.wait()
    tile_copy.wait()

    def merge(step, total):
        for u in range(BUILD):
            at = step * BUILD + u
            keep = plan[2, at].astype(jnp.float32)
            total = total * keep + tiles[plan[1, at]].astype(jnp.float32)
            weights[at] = jnp.transpose(total.astype(weights.dtype))
        return total

    steps = slots // BUILD
    share = steps // n_z
    running = jnp.zeros((edge, edge), jnp.float32)
    for away in range(2, n_z):
        running = lax.fori_loop((away - 2) * share, (away - 1) * share, merge, running)
        vouched(away)
        spread(0, away)
        if away + 1 < n_z:
            vouch(away + 1)
    for c in range(1, chunks):
        for away in reversed(range(1, n_z)):
            spread(c, away)
    lax.fori_loop(max(n_z - 2, 0) * share, steps, merge, running)

    act = {"Z": relay, "S": near, "X": far, "E": collect}
    for op, p, c, at in order_of():
        act[op](p, c, at)

    for k in range(span):
        out[k] = jnp.transpose(out_turned[k])
    for p in range(2):
        for c in range(chunks):
            for k in range(n_z):
                if n_x > 1:
                    across(p, c, k).wait_send()
                if k:
                    along(p, c, sent_to(k)).wait_send()
            for e in range(n_row - 1):
                reduce_copy(p, c, e).wait_send()


def body(n_row, n_col, demand, tile_data, tile_row, tile_col):
    slots, edge = tile_data.shape[2], tile_data.shape[-1]
    columns = demand.shape[1]
    span = demand.shape[0] // edge
    local_rows = n_row * span
    n_x = 2 if n_col % 2 == 0 else 1
    n_z = n_col // n_x
    part = columns // CHUNKS
    width = -(-max(local_rows * n_col * span, slots) // 128) * 128
    dma = pltpu.SemaphoreType.DMA
    kind = demand.dtype
    vmem = pl.BlockSpec(memory_space=pltpu.VMEM)
    result = pl.pallas_call(
        functools.partial(kernel, n_row, n_col, n_x),
        out_shape=jax.ShapeDtypeStruct((span, edge, columns), kind),
        in_specs=[pl.BlockSpec(memory_space=pl.ANY)] * 4,
        out_specs=vmem,
        scratch_shapes=[
            pltpu.VMEM((1, slots), jnp.int32),
            pltpu.VMEM((1, slots), jnp.int32),
            pltpu.VMEM((span, edge, columns), kind),
            pltpu.VMEM((slots, edge, edge), tile_data.dtype),
            pltpu.VMEM((slots + 1, edge, edge), tile_data.dtype),
            pltpu.VMEM((CHUNKS, n_col * span, part, edge), kind),
            pltpu.VMEM((CHUNKS, n_col * span, part, edge), kind),
            pltpu.VMEM((CHUNKS, local_rows, part, edge), jnp.float32),
            pltpu.VMEM((2, CHUNKS, local_rows, part, edge), kind),
            pltpu.VMEM((2, CHUNKS, n_row - 1, span, part, edge), kind),
            pltpu.VMEM((span, columns, edge), kind),
            pltpu.VMEM((8, width), jnp.int32),
            pltpu.SMEM((8, width), jnp.int32),
            pltpu.SemaphoreType.REGULAR((2, n_z + 1)),
            dma((4,)),
            dma,
            dma((2, CHUNKS, n_z)),
            dma((2, CHUNKS, n_z)),
            dma((2, CHUNKS, n_z)),
            dma((2, CHUNKS, n_z)),
            dma((2, CHUNKS, n_row - 1)),
            dma((2, CHUNKS, n_row - 1)),
        ],
        compiler_params=pltpu.CompilerParams(
            collective_id=0, has_side_effects=True, vmem_limit_bytes=28 * 1024 * 1024
        ),
    )(*(
        pltpu.with_memory_space_constraint(operand, pltpu.HBM)
        for operand in (tile_row[0], tile_col[0], demand.reshape(span, edge, columns), tile_data)
    ))
    return result.reshape(demand.shape)


def solution(mesh):
    placed = (
        P(("row", "col"), None),
        P("row", "col", None, None, None),
        P("row", "col", None),
        P("row", "col", None),
    )
    return jax.shard_map(
        functools.partial(body, mesh.shape["row"], mesh.shape["col"]),
        mesh=mesh, in_specs=placed, out_specs=P(("row", "col"), None), check_vma=False,
    )
```
